256 devices in a mesh: cuts: 32 (over z, x), mode: 8 (over y, core).
Axes of the slice: x: 4, y: 4, z: 8, core: 2. Of those that a mesh axis runs over, the one named last changes fastest.
Arguments:
- sliced_state: bfloat16 [8, 64, 4, 128, 2, 128], P(None, 'cuts', None, 'mode'), may hold values from -0.75 to 0.75
- gate_blocks: bfloat16 [32, 2, 128, 128], P('cuts'), may hold values from -0.375 to 0.375
- gate_slot: int32 [32], replicated, may hold values from 0 to 31, each once
- samples: int32 [8, 4096], replicated, may hold values from 0 to 65535
Outputs:
- amplitudes: float32 [32, 128, 2, 128], P('cuts', 'mode')
- sample_probs: float32 [8, 4096], replicated
- xeb_score: float32 [8], replicated
The draws below stay inside these ranges and needn't reach their ends.
Inputs may be any that keep to these rules, and one draw needn't show every extreme that they name: `gate_slot`: a permutation: every gate block has its own row of gate_blocks. `samples`: flat index s * 128 * 128 + p * 128 + q.
All inputs are finite; a program needn't handle non-finite values.
Results may differ from the reference program's by a relative error of at most 0.022.
Values may be sent and summed in bfloat16 or wider, within the bound.
No kernel may reach another device: no remote copies, remote signals or barrier semaphores. Data moves between devices by JAX's collectives and lax.ppermute only.
A program may use at most 64 MiB of HBM per device.

```python
import jax
import jax.numpy as jnp

G = 128
S = 4
CIRC = 8
LAYERS = 2
SAMPLES = 4096
SLICES = 64
NBLK = 32


def plant(entries, rng, smallest, high):
    longest = entries.shape.index(max(entries.shape))
    spots = []
    for shift in (0, 1):
        where = [jax.random.randint(jax.random.fold_in(rng, axis), (), 0, length) for axis, length in enumerate(entries.shape)]
        where[longest] = (where[longest] + shift) % entries.shape[longest]
        spots.append(tuple(where))
    return entries.at[spots[0]].set(smallest).at[spots[1]].set(high)


def steps_of(own_key, extent, shards, smallest, high):
    level, own = 1.0, jax.random.fold_in(own_key, 6)
    for position, blocks in shards:
        steps = jnp.exp(jax.random.uniform(jax.random.fold_in(own, position), (blocks,), jnp.float32, smallest / len(shards), high / len(shards)))
        level = level * jnp.repeat(steps, extent[position] // blocks).reshape([-1 if axis == position else 1 for axis in range(len(extent))])
    return level


def bell_draw(stream_key, dims, deviation, most, split=(), held_as=jnp.bfloat16):
    level = steps_of(stream_key, dims, split, -0.22, 0.18) if split else 1.0
    array = jax.random.normal(stream_key, dims, jnp.float32) * deviation * level
    return jnp.minimum(jnp.maximum(array, -most), most).astype(held_as)


def setup_inputs(seed: int = 0) -> dict:
    arg_keys = jax.random.split(jax.random.key(seed), 5)
    return {
        "sliced_state": bell_draw(arg_keys[0], (CIRC, SLICES, S, G, 2, G), 0.125, 0.75, ((1, 32), (3, 8))),
        "gate_blocks": bell_draw(arg_keys[1], (NBLK, 2, G, G), (2 * G) ** -0.5, 0.375, ((0, 32),)),
        "gate_slot": jax.random.permutation(arg_keys[2], NBLK).astype(jnp.int32),
        "samples": plant(jax.random.randint(arg_keys[3], (CIRC, SAMPLES), 0, S * G * G), jax.random.fold_in(arg_keys[3], 1), 0, (S * G * G) - 1).astype(jnp.int32),
    }


def apply_gates(tensor, blocks):
    real_part = blocks[:, 0]
    imag_part = blocks[:, 1]
    stacked = jnp.concatenate([jnp.concatenate([real_part, imag_part], axis=2), jnp.concatenate([-imag_part, real_part], axis=2)], axis=1)
    layout = tensor.shape
    flattened = tensor.reshape(layout[0], -1, 2 * layout[-1])
    product = jnp.einsum("crk,ckn->crn", flattened.astype(jnp.float32), stacked.astype(jnp.float32))
    return product.astype(jnp.bfloat16).reshape(layout)


def reference(sliced_state, gate_blocks, gate_slot, samples):
    tensor = sliced_state
    circuit_ids = jnp.arange(CIRC, dtype=jnp.int32)
    for layer_index in range(LAYERS):
        for gate_kind in range(2):
            block_ids = (circuit_ids * LAYERS + layer_index) * 2 + gate_kind
            blocks = gate_blocks[gate_slot[block_ids]]
            if gate_kind == 1:
                tensor = jnp.swapaxes(tensor, 3, 5)
            tensor = apply_gates(tensor, blocks)
            if gate_kind == 1:
                tensor = jnp.swapaxes(tensor, 3, 5)
    amplitudes = jnp.sum(tensor.astype(jnp.float32), axis=1).reshape(CIRC * S, G, 2, G)
    magnitude = amplitudes[:, :, 0, :] ** 2 + amplitudes[:, :, 1, :] ** 2
    per_circuit = magnitude.reshape(CIRC, S * G * G)
    norm_total = jnp.sum(per_circuit, axis=1)
    picked = jnp.take_along_axis(per_circuit, samples, axis=1)
    sample_probs = picked * float(S * G * G) / norm_total[:, None]
    xeb_score = jnp.mean(sample_probs, axis=1)
    return amplitudes, sample_probs, xeb_score
```

```python
import functools

import jax
import jax.numpy as jnp
from jax import lax
from jax.experimental import pallas as pl
from jax.experimental.pallas import tpu as pltpu
from jax.sharding import Mesh
from jax.sharding import PartitionSpec as P

BF, F32, I32 = jnp.bfloat16, jnp.float32, jnp.int32
Z, X, Y, K = 8, 4, 4, 2
M = Y * K
W = 128
VM = pl.BlockSpec(memory_space=pltpu.VMEM)
SM = pl.BlockSpec(memory_space=pltpu.SMEM)


def mode_index():
    return lax.axis_index("y") * K + lax.axis_index("k")


def dot(a, b):
    return jnp.dot(a, b, preferred_element_type=F32)


def pack_kernel(state_ref, gates_ref, out_ref):
    mode = mode_index()
    for c in range(Z):
        for s in range(X):
            total = state_ref[c, 0, s].astype(F32) + state_ref[c, 1, s].astype(F32)
            out_ref[c * X + s, 0:32, :] = total.astype(BF)
    for s in range(X):
        start = pl.multiple_of((s * M + mode) * 8, 8)
        rows = gates_ref[pl.ds(start, 8), :]
        for c in range(Z):
            out_ref[c * X + s, 32:40, :] = rows


def sum_kernel(slot_ref, in_ref, out_ref, sum_ref):
    circuit = lax.axis_index("z")
    total = in_ref[0, 0:32, :].astype(F32)
    for i in range(1, Z * X):
        total = total + in_ref[i, 0:32, :].astype(F32)
    sum_ref[...] = total
    state = jnp.concatenate([sum_ref[pl.ds(0, 16, stride=2), :], sum_ref[pl.ds(1, 16, stride=2), :]], axis=0).astype(BF)
    gates = [in_ref[slot_ref[circuit * 4 + b], 32:40, :] for b in range(4)]
    for i in range(X * M):
        out_ref[i, 0:32, :] = state
        for b in range(4):
            out_ref[i, 32 + 8 * b : 40 + 8 * b, :] = gates[b]


def embed(real, imag):
    return jnp.concatenate([jnp.concatenate([real, imag], axis=1), jnp.concatenate([-imag, real], axis=1)], axis=0)


def compose(first, second):
    left = jnp.concatenate([first[:W], first[W:]], axis=1)
    return dot(left, embed(second[:W], second[W:]))


def apply_kernel(samples_ref, in_ref, amp_ref, out_ref, full_ref, pick_ref):
    circuit = lax.axis_index("z")
    spect = lax.axis_index("x")
    mode = mode_index()
    g = [in_ref[:, 32 + 8 * b : 40 + 8 * b, :].reshape(2 * W, W) for b in range(4)]
    col = compose(g[0], g[2]).astype(BF)
    row = compose(g[1], g[3])
    row_r, row_i = row[:, :W].T.astype(BF), row[:, W:].T.astype(BF)
    gate_q = embed(col[:, :W], col[:, W:])
    gate_p = jnp.concatenate([jnp.concatenate([row_r, -row_i], axis=1), jnp.concatenate([row_i, row_r], axis=1)], axis=0)
    real = in_ref[:, 0:16, :].reshape(X * W, W)
    imag = in_ref[:, 16:32, :].reshape(X * W, W)
    mid = dot(jnp.concatenate([real, imag], axis=1), gate_q).astype(BF)
    mid = jnp.concatenate(
        [jnp.concatenate([mid[s * W : (s + 1) * W, r * W : (r + 1) * W] for s in range(X)], axis=1) for r in range(2)], axis=0
    )
    full = dot(gate_p, mid)
    for s in range(X):
        for r in range(2):
            full_ref[s, r] = full[r * W : (r + 1) * W, s * W : (s + 1) * W]
    start = pl.multiple_of(mode * 16, 16)
    for r in range(2):
        amp_ref[0, :, r, :] = full_ref[spect, r, pl.ds(start, 16), :]
    mag = full[:W] * full[:W] + full[W:] * full[W:]
    norm = jnp.sum(mag)
    table = jnp.concatenate([mag[:, : 2 * W], mag[:, 2 * W :]], axis=0).astype(BF)
    chunk = 512
    for j in range(4096 // chunk):
        flat = samples_ref[pl.ds(circuit, 1), j * chunk : (j + 1) * chunk]
        lane = ((flat >> 14) & 1) * W + (flat & 127)
        line = ((flat >> 15) & 1) * W + ((flat >> 7) & 127)
        ids = lax.broadcasted_iota(I32, (2 * W, chunk), 0)
        onehot = jnp.where(ids == lane, 1.0, 0.0).astype(BF)
        got = dot(table, onehot)
        got = jnp.sum(jnp.where(ids == line, got, 0.0), axis=0, keepdims=True)
        for i in range(chunk // W):
            pick_ref[j * (chunk // W) + i : j * (chunk // W) + i + 1, :] = got[:, i * W : (i + 1) * W]
    picked = pick_ref[...].astype(BF)
    tail = jnp.full((8, W), norm, F32)
    high = tail.astype(BF).astype(F32)
    tail = jnp.where(lax.broadcasted_iota(I32, (8, W), 0) == 0, high, tail - high).astype(BF)
    for c in range(Z):
        out_ref[c, 0:32, :] = picked
        out_ref[c, 32:40, :] = tail


def finish_kernel(in_ref, probs_ref, score_ref, wide_ref):
    for c in range(Z):
        tail = in_ref[c, 32:40, :].astype(F32)
        norm = tail[0:1] + tail[1:2]
        wide_ref[c * 32 : (c + 1) * 32, :] = in_ref[c, 0:32, :].astype(F32) * 65536.0 / norm
    total = jnp.zeros((Z, W), F32)
    for j in range(32):
        rows = wide_ref[pl.ds(j, Z, stride=32), :]
        probs_ref[:, j * W : (j + 1) * W] = rows
        total = total + rows
    score = jnp.sum(total, axis=1, keepdims=True) * (1.0 / 4096.0)
    diag = lax.broadcasted_iota(I32, (Z, W), 0) == lax.broadcasted_iota(I32, (Z, W), 1)
    score_ref[...] = jnp.sum(jnp.where(diag, score, 0.0), axis=0, keepdims=True)[:, :Z]


def exchange(array, axes):
    return lax.all_to_all(array, axes, split_axis=0, concat_axis=0, tiled=True)


def on_device(sliced_state, gate_blocks, gate_slot, samples):
    shape = jax.ShapeDtypeStruct
    state = sliced_state.reshape(Z, 2, X, 32, W)
    packed = pl.pallas_call(pack_kernel, out_shape=shape((Z * X, 40, W), BF), in_specs=[VM, VM], out_specs=VM, name="pack")(
        state, gate_blocks.reshape(2 * W, W)
    )
    packed = exchange(packed, ("z", "x"))
    plane = pl.pallas_call(
        sum_kernel,
        out_shape=shape((X * M, 64, W), BF),
        in_specs=[SM, VM],
        out_specs=VM,
        scratch_shapes=[pltpu.VMEM((32, W), F32)],
        name="sum",
    )(gate_slot, packed)
    plane = exchange(plane, ("x", "y", "k"))
    amplitudes, picked = pl.pallas_call(
        apply_kernel,
        out_shape=(shape((1, 16, 2, W), F32), shape((Z, 40, W), BF)),
        in_specs=[VM, VM],
        out_specs=(VM, VM),
        scratch_shapes=[pltpu.VMEM((X, 2, W, W), F32), pltpu.VMEM((32, W), F32)],
        name="apply",
    )(samples, plane)
    picked = exchange(picked, "z")
    probs, score = pl.pallas_call(
        finish_kernel,
        out_shape=(shape((Z, 4096), F32), shape((1, Z), F32)),
        in_specs=[VM],
        out_specs=(VM, VM),
        scratch_shapes=[pltpu.VMEM((Z * 32, W), F32)],
        name="finish",
    )(picked)
    return amplitudes, probs, score.reshape(Z)


def solution(mesh):
    split = Mesh(mesh.devices.reshape(Z, X, Y, K), ("z", "x", "y", "k"))
    placed = (P(None, ("z", "x"), None, ("y", "k"), None, None), P(("z", "x"), None, None, None), P(), P())
    return jax.shard_map(
        on_device,
        mesh=split,
        in_specs=placed,
        out_specs=(P(("z", "x"), ("y", "k"), None, None), P(), P()),
        check_vma=False,
    )
```

```python
import functools

import jax
import jax.numpy as jnp
from jax import lax
from jax.experimental import pallas as pl
from jax.experimental.pallas import tpu as pltpu
from jax.sharding import Mesh
from jax.sharding import PartitionSpec as P

BF, F32, I32 = jnp.bfloat16, jnp.float32, jnp.int32
Z, X, Y, K = 8, 4, 4, 2
M = Y * K
W = 128
CP = pltpu.CompilerParams(vmem_limit_bytes=8 * 2**20)
VM = pl.BlockSpec(memory_space=pltpu.VMEM)
HB = pl.BlockSpec(memory_space=pltpu.HBM)
SM = pl.BlockSpec(memory_space=pltpu.SMEM)


def mode_index():
    return lax.axis_index("y") * K + lax.axis_index("k")


def dot(a, b):
    return jnp.dot(a, b, preferred_element_type=F32)


def pack_kernel(state_ref, gates_ref, out_ref, held_ref, rows_ref, sems):
    copies = [pltpu.make_async_copy(state_ref.at[c], held_ref.at[c], sems.at[c]) for c in range(Z)]
    for copy in copies:
        copy.start()
    rows = pltpu.make_async_copy(gates_ref.at[:, mode_index()], rows_ref, sems.at[Z])
    rows.start()
    for c in range(Z):
        copies[c].wait()
        for s in range(X):
            total = held_ref[c, 0, s].astype(F32) + held_ref[c, 1, s].astype(F32)
            out_ref[c * X + s, 0:32, :] = total.astype(BF)
    rows.wait()
    for s in range(X):
        for c in range(Z):
            out_ref[c * X + s, 32:40, :] = rows_ref[s]


def sum_kernel(slot_ref, in_ref, out_ref, sum_ref):
    circuit = lax.axis_index("z")
    total = in_ref[0, 0:32, :].astype(F32)
    for i in range(1, Z * X):
        total = total + in_ref[i, 0:32, :].astype(F32)
    sum_ref[...] = total
    state = jnp.concatenate([sum_ref[pl.ds(0, 16, stride=2), :], sum_ref[pl.ds(1, 16, stride=2), :]], axis=0).astype(BF)
    gates = [in_ref[slot_ref[circuit * 4 + b], 32:40, :] for b in range(4)]
    for i in range(X * Y):
        out_ref[i, 0:32, :] = state
        for b in range(4):
            out_ref[i, 32 + 8 * b : 40 + 8 * b, :] = gates[b]


def embed(real, imag):
    return jnp.concatenate([jnp.concatenate([real, imag], axis=1), jnp.concatenate([-imag, real], axis=1)], axis=0)


def compose(first, second):
    left = jnp.concatenate([first[:W], first[W:]], axis=1)
    return dot(left, embed(second[:W], second[W:]))


def apply_kernel(samples_ref, own_ref, pair_ref, amp_ref, out_ref, in_ref, full_ref, pick_ref):
    circuit = lax.axis_index("z")
    spect = lax.axis_index("x")
    core = lax.axis_index("k")
    mode = mode_index()
    in_ref[:, core] = own_ref[...]
    in_ref[:, 1 - core] = pair_ref[...]
    g = [in_ref[:, :, 32 + 8 * b : 40 + 8 * b, :].reshape(2 * W, W) for b in range(4)]
    col = compose(g[0], g[2]).astype(BF)
    row = compose(g[1], g[3])
    row_r, row_i = row[:, :W].T.astype(BF), row[:, W:].T.astype(BF)
    gate_q = embed(col[:, :W], col[:, W:])
    gate_p = jnp.concatenate([jnp.concatenate([row_r, -row_i], axis=1), jnp.concatenate([row_i, row_r], axis=1)], axis=0)
    real = in_ref[:, :, 0:16, :].reshape(X * W, W)
    imag = in_ref[:, :, 16:32, :].reshape(X * W, W)
    mid = dot(jnp.concatenate([real, imag], axis=1), gate_q).astype(BF)
    mid = jnp.concatenate(
        [jnp.concatenate([mid[s * W : (s + 1) * W, r * W : (r + 1) * W] for s in range(X)], axis=1) for r in range(2)], axis=0
    )
    full = dot(gate_p, mid)
    for s in range(X):
        for r in range(2):
            full_ref[s, r] = full[r * W : (r + 1) * W, s * W : (s + 1) * W]
    start = pl.multiple_of(mode * 16, 16)
    for r in range(2):
        amp_ref[0, :, r, :] = full_ref[spect, r, pl.ds(start, 16), :]
    mag = full[:W] * full[:W] + full[W:] * full[W:]
    norm = jnp.sum(mag)
    table = jnp.concatenate([mag[:, : 2 * W], mag[:, 2 * W :]], axis=0).astype(BF)
    chunk = 512
    for j in range(4096 // chunk):
        flat = samples_ref[pl.ds(circuit, 1), j * chunk : (j + 1) * chunk]
        lane = ((flat >> 14) & 1) * W + (flat & 127)
        line = ((flat >> 15) & 1) * W + ((flat >> 7) & 127)
        ids = lax.broadcasted_iota(I32, (2 * W, chunk), 0)
        onehot = jnp.where(ids == lane, 1.0, 0.0).astype(BF)
        got = dot(table, onehot)
        got = jnp.sum(jnp.where(ids == line, got, 0.0), axis=0, keepdims=True)
        for i in range(chunk // W):
            pick_ref[j * (chunk // W) + i : j * (chunk // W) + i + 1, :] = got[:, i * W : (i + 1) * W]
    picked = pick_ref[...].astype(BF)
    tail = jnp.full((8, W), norm, F32)
    high = tail.astype(BF).astype(F32)
    tail = jnp.where(lax.broadcasted_iota(I32, (8, W), 0) == 0, high, tail - high).astype(BF)
    for c in range(Z):
        out_ref[c, 0:32, :] = picked
        out_ref[c, 32:40, :] = tail


def finish_kernel(in_ref, probs_ref, score_ref, wide_ref):
    for c in range(Z):
        tail = in_ref[c, 32:40, :].astype(F32)
        norm = tail[0:1] + tail[1:2]
        wide_ref[c * 32 : (c + 1) * 32, :] = in_ref[c, 0:32, :].astype(F32) * 65536.0 / norm
    total = jnp.zeros((Z, W), F32)
    for j in range(32):
        rows = wide_ref[pl.ds(j, Z, stride=32), :]
        probs_ref[:, j * W : (j + 1) * W] = rows
        total = total + rows
    score = jnp.sum(total, axis=1, keepdims=True) * (1.0 / 4096.0)
    diag = lax.broadcasted_iota(I32, (Z, W), 0) == lax.broadcasted_iota(I32, (Z, W), 1)
    score_ref[...] = jnp.sum(jnp.where(diag, score, 0.0), axis=0, keepdims=True)[:, :Z]


def hbm(array):
    return pltpu.with_memory_space_constraint(array, pltpu.HBM)


def exchange(array, axes):
    return lax.all_to_all(array, axes, split_axis=0, concat_axis=0, tiled=True)


def on_device(sliced_state, gate_blocks, gate_slot, samples):
    shape = jax.ShapeDtypeStruct
    state = sliced_state.reshape(Z, 2, X, 32, W)
    packed = pl.pallas_call(pack_kernel, out_shape=shape((Z * X, 40, W), BF), in_specs=[HB, HB], out_specs=VM, compiler_params=CP, name="pack",
        scratch_shapes=[pltpu.VMEM((Z, 2, X, 32, W), BF), pltpu.VMEM((X, 8, W), BF), pltpu.SemaphoreType.DMA((Z + 1,))])(
        hbm(state), hbm(gate_blocks.reshape(X, M, 8, W))
    )
    packed = exchange(packed, ("z", "x"))
    plane = pl.pallas_call(
        sum_kernel,
        out_shape=shape((X * Y, 64, W), BF),
        in_specs=[SM, VM],
        out_specs=VM,
        scratch_shapes=[pltpu.VMEM((32, W), F32)],
        compiler_params=CP, name="sum",
    )(gate_slot, packed)
    plane = exchange(plane, ("x", "y"))
    pair = lax.ppermute(plane, "k", [(0, 1), (1, 0)])
    amplitudes, picked = pl.pallas_call(
        apply_kernel,
        out_shape=(shape((1, 16, 2, W), F32), shape((Z, 40, W), BF)),
        in_specs=[VM, VM, VM],
        out_specs=(VM, VM),
        scratch_shapes=[pltpu.VMEM((X * Y, K, 64, W), BF), pltpu.VMEM((X, 2, W, W), F32), pltpu.VMEM((32, W), F32)],
        compiler_params=CP, name="apply",
    )(samples, plane, pair)
    picked = exchange(picked, "z")
    probs, score = pl.pallas_call(
        finish_kernel,
        out_shape=(shape((Z, 4096), F32), shape((1, Z), F32)),
        in_specs=[VM],
        out_specs=(VM, VM),
        scratch_shapes=[pltpu.VMEM((Z * 32, W), F32)],
        compiler_params=CP, name="finish",
    )(picked)
    return amplitudes, probs, score.reshape(Z)


def solution(mesh):
    split = Mesh(mesh.devices.reshape(Z, X, Y, K), ("z", "x", "y", "k"))
    placed = (P(None, ("z", "x"), None, ("y", "k"), None, None), P(("z", "x"), None, None, None), P(), P())
    return jax.shard_map(
        on_device,
        mesh=split,
        in_specs=placed,
        out_specs=(P(("z", "x"), ("y", "k"), None, None), P(), P()),
        check_vma=False,
    )
```

```python
import functools

import jax
import jax.numpy as jnp
from jax import lax
from jax.experimental import pallas as pl
from jax.experimental.pallas import tpu as pltpu
from jax.sharding import Mesh
from jax.sharding import PartitionSpec as P

BF, F32, I32 = jnp.bfloat16, jnp.float32, jnp.int32
Z, X, Y, K = 8, 4, 4, 2
M = Y * K
W = 128
Z_FIRST, X_FIRST, Y_FIRST = 4, 2, 2
CP = pltpu.CompilerParams(vmem_limit_bytes=8 * 2**20)
VM = pl.BlockSpec(memory_space=pltpu.VMEM)
HB = pl.BlockSpec(memory_space=pltpu.HBM)
SM = pl.BlockSpec(memory_space=pltpu.SMEM)


def led_by(first, count):
    return [first] + [i for i in range(count) if i != first]


Z_ORDER, X_ORDER, Y_ORDER = led_by(Z_FIRST, Z), led_by(X_FIRST, X), led_by(Y_FIRST, Y)
ZX_ORDER = [z * X + x for z in Z_ORDER for x in X_ORDER]
XY_ORDER = [x * Y + y for x in X_ORDER for y in Y_ORDER]


def place(index, first):
    return jnp.where(index == first, 0, jnp.where(index < first, index + 1, index))


def mode_index():
    return lax.axis_index("y") * K + lax.axis_index("k")


def dot(a, b):
    return jnp.dot(a, b, preferred_element_type=F32)


def pack_kernel(state_ref, gates_ref, out_ref, held_ref, rows_ref, sems):
    copies = [pltpu.make_async_copy(state_ref.at[c], held_ref.at[c], sems.at[c]) for c in range(Z)]
    for copy in copies:
        copy.start()
    rows = pltpu.make_async_copy(gates_ref.at[:, mode_index()], rows_ref, sems.at[Z])
    rows.start()
    for c in range(Z):
        copies[c].wait()
        for s in range(X):
            total = held_ref[c, 0, s].astype(F32) + held_ref[c, 1, s].astype(F32)
            out_ref[ZX_ORDER.index(c * X + s), 0:32, :] = total.astype(BF)
    rows.wait()
    for s in range(X):
        for c in range(Z):
            out_ref[ZX_ORDER.index(c * X + s), 32:40, :] = rows_ref[s]


def sum_kernel(slot_ref, in_ref, out_ref, sum_ref):
    circuit = lax.axis_index("z")
    total = in_ref[0, 0:32, :].astype(F32)
    for i in range(1, Z * X):
        total = total + in_ref[i, 0:32, :].astype(F32)
    sum_ref[...] = total
    state = jnp.concatenate([sum_ref[pl.ds(0, 16, stride=2), :], sum_ref[pl.ds(1, 16, stride=2), :]], axis=0).astype(BF)
    slots = [slot_ref[circuit * 4 + b] for b in range(4)]
    gates = [in_ref[place(slot // X, Z_FIRST) * X + place(slot % X, X_FIRST), 32:40, :] for slot in slots]
    for i in range(X * Y):
        out_ref[i, 0:32, :] = state
        for b in range(4):
            out_ref[i, 32 + 8 * b : 40 + 8 * b, :] = gates[b]


def embed(real, imag):
    return jnp.concatenate([jnp.concatenate([real, imag], axis=1), jnp.concatenate([-imag, real], axis=1)], axis=0)


def compose(first, second):
    left = jnp.concatenate([first[:W], first[W:]], axis=1)
    return dot(left, embed(second[:W], second[W:]))


def apply_kernel(samples_ref, own_ref, pair_ref, amp_ref, out_ref, in_ref, full_ref, pick_ref):
    circuit = lax.axis_index("z")
    spect = lax.axis_index("x")
    core = lax.axis_index("k")
    mode = mode_index()
    for i, at in enumerate(XY_ORDER):
        in_ref[at, core] = own_ref[i]
        in_ref[at, 1 - core] = pair_ref[i]
    g = [in_ref[:, :, 32 + 8 * b : 40 + 8 * b, :].reshape(2 * W, W) for b in range(4)]
    col = compose(g[0], g[2]).astype(BF)
    row = compose(g[1], g[3])
    row_r, row_i = row[:, :W].T.astype(BF), row[:, W:].T.astype(BF)
    gate_q = embed(col[:, :W], col[:, W:])
    gate_p = jnp.concatenate([jnp.concatenate([row_r, -row_i], axis=1), jnp.concatenate([row_i, row_r], axis=1)], axis=0)
    real = in_ref[:, :, 0:16, :].reshape(X * W, W)
    imag = in_ref[:, :, 16:32, :].reshape(X * W, W)
    mid = dot(jnp.concatenate([real, imag], axis=1), gate_q).astype(BF)
    mid = jnp.concatenate(
        [jnp.concatenate([mid[s * W : (s + 1) * W, r * W : (r + 1) * W] for s in range(X)], axis=1) for r in range(2)], axis=0
    )
    full = dot(gate_p, mid)
    for s in range(X):
        for r in range(2):
            full_ref[s, r] = full[r * W : (r + 1) * W, s * W : (s + 1) * W]
    start = pl.multiple_of(mode * 16, 16)
    for r in range(2):
        amp_ref[0, :, r, :] = full_ref[spect, r, pl.ds(start, 16), :]
    mag = full[:W] * full[:W] + full[W:] * full[W:]
    norm = jnp.sum(mag)
    table = jnp.concatenate([mag[:, : 2 * W], mag[:, 2 * W :]], axis=0).astype(BF)
    chunk = 512
    for j in range(4096 // chunk):
        flat = samples_ref[pl.ds(circuit, 1), j * chunk : (j + 1) * chunk]
        lane = ((flat >> 14) & 1) * W + (flat & 127)
        line = ((flat >> 15) & 1) * W + ((flat >> 7) & 127)
        ids = lax.broadcasted_iota(I32, (2 * W, chunk), 0)
        onehot = jnp.where(ids == lane, 1.0, 0.0).astype(BF)
        got = dot(table, onehot)
        got = jnp.sum(jnp.where(ids == line, got, 0.0), axis=0, keepdims=True)
        for i in range(chunk // W):
            pick_ref[j * (chunk // W) + i : j * (chunk // W) + i + 1, :] = got[:, i * W : (i + 1) * W]
    picked = pick_ref[...].astype(BF)
    tail = jnp.full((8, W), norm, F32)
    high = tail.astype(BF).astype(F32)
    tail = jnp.where(lax.broadcasted_iota(I32, (8, W), 0) == 0, high, tail - high).astype(BF)
    for c in range(Z):
        out_ref[c, 0:32, :] = picked
        out_ref[c, 32:40, :] = tail


def finish_kernel(in_ref, held_ref, probs_ref, score_ref, amp_ref, wide_ref):
    amp_ref[...] = held_ref[...]
    for i, c in enumerate(Z_ORDER):
        tail = in_ref[i, 32:40, :].astype(F32)
        norm = tail[0:1] + tail[1:2]
        wide_ref[c * 32 : (c + 1) * 32, :] = in_ref[i, 0:32, :].astype(F32) * 65536.0 / norm
    total = jnp.zeros((Z, W), F32)
    for j in range(32):
        rows = wide_ref[pl.ds(j, Z, stride=32), :]
        probs_ref[:, j * W : (j + 1) * W] = rows
        total = total + rows
    score = jnp.sum(total, axis=1, keepdims=True) * (1.0 / 4096.0)
    diag = lax.broadcasted_iota(I32, (Z, W), 0) == lax.broadcasted_iota(I32, (Z, W), 1)
    score_ref[...] = jnp.sum(jnp.where(diag, score, 0.0), axis=0, keepdims=True)[:, :Z]


def hbm(array):
    return pltpu.with_memory_space_constraint(array, pltpu.HBM)


def exchange(array, axes, order):
    return lax.all_to_all(array, axes, split_axis=0, concat_axis=0, tiled=True, axis_index_groups=[order])


def on_device(sliced_state, gate_blocks, gate_slot, samples):
    shape = jax.ShapeDtypeStruct
    state = sliced_state.reshape(Z, 2, X, 32, W)
    packed = pl.pallas_call(pack_kernel, out_shape=shape((Z * X, 40, W), BF), in_specs=[HB, HB], out_specs=VM, compiler_params=CP, name="pack",
        scratch_shapes=[pltpu.VMEM((Z, 2, X, 32, W), BF), pltpu.VMEM((X, 8, W), BF), pltpu.SemaphoreType.DMA((Z + 1,))])(
        hbm(state), hbm(gate_blocks.reshape(X, M, 8, W))
    )
    packed = exchange(packed, ("z", "x"), ZX_ORDER)
    plane = pl.pallas_call(
        sum_kernel,
        out_shape=shape((X * Y, 64, W), BF),
        in_specs=[SM, VM],
        out_specs=VM,
        scratch_shapes=[pltpu.VMEM((32, W), F32)],
        compiler_params=CP, name="sum",
    )(gate_slot, packed)
    plane = exchange(plane, ("x", "y"), XY_ORDER)
    pair = lax.ppermute(plane, "k", [(0, 1), (1, 0)])
    amplitudes, picked = pl.pallas_call(
        apply_kernel,
        out_shape=(shape((1, 16, 2, W), F32), shape((Z, 40, W), BF)),
        in_specs=[VM, VM, VM],
        out_specs=(VM, VM),
        scratch_shapes=[pltpu.VMEM((X * Y, K, 64, W), BF), pltpu.VMEM((X, 2, W, W), F32), pltpu.VMEM((32, W), F32)],
        compiler_params=CP, name="apply",
    )(samples, plane, pair)
    picked = exchange(picked, "z", Z_ORDER)
    probs, score, amplitudes = pl.pallas_call(
        finish_kernel,
        out_shape=(shape((Z, 4096), F32), shape((1, Z), F32), shape((1, 16, 2, W), F32)),
        in_specs=[VM, VM],
        out_specs=(VM, VM, VM),
        scratch_shapes=[pltpu.VMEM((Z * 32, W), F32)],
        compiler_params=CP, name="finish",
    )(picked, amplitudes)
    return amplitudes, probs, score.reshape(Z)


def solution(mesh):
    split = Mesh(mesh.devices.reshape(Z, X, Y, K), ("z", "x", "y", "k"))
    placed = (P(None, ("z", "x"), None, ("y", "k"), None, None), P(("z", "x"), None, None, None), P(), P())
    return jax.shard_map(
        on_device,
        mesh=split,
        in_specs=placed,
        out_specs=(P(("z", "x"), ("y", "k"), None, None), P(), P()),
        check_vma=False,
    )
```

```python
import functools

import jax
import jax.numpy as jnp
from jax import lax
from jax.experimental import pallas as pl
from jax.experimental.pallas import tpu as pltpu
from jax.sharding import Mesh
from jax.sharding import PartitionSpec as P

BF, F32, I32 = jnp.bfloat16, jnp.float32, jnp.int32
Z, X, Y, K = 8, 4, 4, 2
M = Y * K
W = 128
Z_FIRST, X_FIRST, Y_FIRST = 4, 2, 2
CP = pltpu.CompilerParams(vmem_limit_bytes=8 * 2**20)
VM = pl.BlockSpec(memory_space=pltpu.VMEM)
ANY = pl.BlockSpec(memory_space=pl.ANY)
HB = pl.BlockSpec(memory_space=pltpu.HBM)


def led_by(first, count):
    return [first] + [i for i in range(count) if i != first]


Z_ORDER, X_ORDER, Y_ORDER = led_by(Z_FIRST, Z), led_by(X_FIRST, X), led_by(Y_FIRST, Y)
ZX_ORDER = [z * X + x for z in Z_ORDER for x in X_ORDER]
XY_ORDER = [x * Y + y for y in Y_ORDER for x in X_ORDER]


def mode_index():
    return lax.axis_index("y") * K + lax.axis_index("k")


def dot(a, b):
    return jnp.dot(a, b, preferred_element_type=F32)


def pack_kernel(state_ref, gates_ref, slot_ref, out_ref, slot_out_ref, held_ref, rows_ref, sems):
    copies = [pltpu.make_async_copy(state_ref.at[c], held_ref.at[c], sems.at[c]) for c in range(Z)]
    for copy in copies:
        copy.start()
    rows = pltpu.make_async_copy(gates_ref.at[:, mode_index()], rows_ref, sems.at[Z])
    rows.start()
    slots = pltpu.make_async_copy(slot_ref, slot_out_ref, sems.at[Z + 1])
    slots.start()
    for c in range(Z):
        copies[c].wait()
        for s in range(X):
            total = held_ref[c, 0, s].astype(F32) + held_ref[c, 1, s].astype(F32)
            out_ref[ZX_ORDER.index(c * X + s), 0:32, :] = total.astype(BF)
    rows.wait()
    slots.wait()
    for s in range(X):
        for c in range(Z):
            out_ref[ZX_ORDER.index(c * X + s), 32:40, :] = rows_ref[s]


def sum_kernel(slot_ref, in_ref, out_ref, sum_ref):
    first = lax.axis_index("z") * 4
    slots = jnp.broadcast_to(slot_ref[...], (8, Z * X))
    blocks = lax.broadcasted_iota(I32, (8, Z * X), 1) - first
    wanted = [jnp.sum(jnp.where(blocks == b, slots, 0), axis=1, keepdims=True) for b in range(4)]
    total = jnp.zeros((32, W), F32)
    gates = [jnp.zeros((8, W), F32) for _ in range(4)]
    for i, owner in enumerate(ZX_ORDER):
        total = total + in_ref[i, 0:32, :].astype(F32)
        rows = in_ref[i, 32:40, :].astype(F32)
        gates = [jnp.where(wanted[b] == owner, rows, gates[b]) for b in range(4)]
    sum_ref[...] = total
    state = jnp.concatenate([sum_ref[pl.ds(0, 16, stride=2), :], sum_ref[pl.ds(1, 16, stride=2), :]], axis=0).astype(BF)
    for i in range(X * Y):
        out_ref[i, 0:32, :] = state
        for b in range(4):
            out_ref[i, 32 + 8 * b : 40 + 8 * b, :] = gates[b].astype(BF)


def embed(real, imag):
    return jnp.concatenate([jnp.concatenate([real, imag], axis=1), jnp.concatenate([-imag, real], axis=1)], axis=0)


def compose(first, second):
    left = jnp.concatenate([first[:W], first[W:]], axis=1)
    return dot(left, embed(second[:W], second[W:]))


def hot_kernel(samples_ref, after_ref, out_ref):
    flat = samples_ref[pl.ds(lax.axis_index("z"), 1), :]
    lane = (((flat >> 14) & 1) * W + (flat & 127)).astype(F32).astype(BF)
    chunk = 512
    ids = lax.broadcasted_iota(I32, (2 * W, chunk), 0).astype(F32).astype(BF)
    for j in range(4096 // chunk):
        hit = ids == lane[:, j * chunk : (j + 1) * chunk]
        out_ref[:, j * chunk : (j + 1) * chunk] = jnp.where(hit, jnp.ones((), BF), jnp.zeros((), BF))


def apply_kernel(samples_ref, hot_ref, own_ref, pair_ref, amp_ref, out_ref, in_ref, full_ref, pick_ref):
    circuit = lax.axis_index("z")
    spect = lax.axis_index("x")
    core = lax.axis_index("k")
    mode = mode_index()
    for i, at in enumerate(XY_ORDER):
        in_ref[at, core] = own_ref[i]
        in_ref[at, 1 - core] = pair_ref[i]
    g = [in_ref[:, :, 32 + 8 * b : 40 + 8 * b, :].reshape(2 * W, W) for b in range(4)]
    col = compose(g[0], g[2]).astype(BF)
    row = compose(g[1], g[3])
    row_r, row_i = row[:, :W].T.astype(BF), row[:, W:].T.astype(BF)
    gate_q = embed(col[:, :W], col[:, W:])
    gate_p = jnp.concatenate([jnp.concatenate([row_r, -row_i], axis=1), jnp.concatenate([row_i, row_r], axis=1)], axis=0)
    real = in_ref[:, :, 0:16, :].reshape(X * W, W)
    imag = in_ref[:, :, 16:32, :].reshape(X * W, W)
    mid = dot(jnp.concatenate([real, imag], axis=1), gate_q).astype(BF)
    mid = jnp.concatenate(
        [jnp.concatenate([mid[s * W : (s + 1) * W, r * W : (r + 1) * W] for s in range(X)], axis=1) for r in range(2)], axis=0
    )
    full = dot(gate_p, mid)
    for s in range(X):
        for r in range(2):
            full_ref[s, r] = full[r * W : (r + 1) * W, s * W : (s + 1) * W]
    start = pl.multiple_of(mode * 16, 16)
    for r in range(2):
        amp_ref[0, :, r, :] = full_ref[spect, r, pl.ds(start, 16), :]
    mag = full[:W] * full[:W] + full[W:] * full[W:]
    norm = jnp.sum(mag)
    table = jnp.concatenate([mag[:, : 2 * W], mag[:, 2 * W :]], axis=0).astype(BF)
    chunk = 512
    for j in range(4096 // chunk):
        flat = samples_ref[pl.ds(circuit, 1), j * chunk : (j + 1) * chunk]
        line = ((flat >> 15) & 1) * W + ((flat >> 7) & 127)
        ids = lax.broadcasted_iota(I32, (2 * W, chunk), 0)
        got = dot(table, hot_ref[:, j * chunk : (j + 1) * chunk])
        got = jnp.sum(jnp.where(ids == line, got, 0.0), axis=0, keepdims=True)
        for i in range(chunk // W):
            pick_ref[j * (chunk // W) + i : j * (chunk // W) + i + 1, :] = got[:, i * W : (i + 1) * W]
    picked = pick_ref[...].astype(BF)
    tail = jnp.full((8, W), norm, F32)
    high = tail.astype(BF).astype(F32)
    tail = jnp.where(lax.broadcasted_iota(I32, (8, W), 0) == 0, high, tail - high).astype(BF)
    for c in range(Z):
        out_ref[c, 0:32, :] = picked
        out_ref[c, 32:40, :] = tail


def finish_kernel(in_ref, held_ref, probs_ref, score_ref, amp_ref, wide_ref):
    amp_ref[...] = held_ref[...]
    for i, c in enumerate(Z_ORDER):
        tail = in_ref[i, 32:40, :].astype(F32)
        norm = tail[0:1] + tail[1:2]
        wide_ref[c * 32 : (c + 1) * 32, :] = in_ref[i, 0:32, :].astype(F32) * 65536.0 / norm
    total = jnp.zeros((Z, W), F32)
    for j in range(32):
        rows = wide_ref[pl.ds(j, Z, stride=32), :]
        probs_ref[:, j * W : (j + 1) * W] = rows
        total = total + rows
    score = jnp.sum(total, axis=1, keepdims=True) * (1.0 / 4096.0)
    diag = lax.broadcasted_iota(I32, (Z, W), 0) == lax.broadcasted_iota(I32, (Z, W), 1)
    score_ref[...] = jnp.sum(jnp.where(diag, score, 0.0), axis=0, keepdims=True)[:, :Z]


def hbm(array):
    return pltpu.with_memory_space_constraint(array, pltpu.HBM)


def exchange(array, axes, order):
    return lax.all_to_all(array, axes, split_axis=0, concat_axis=0, tiled=True, axis_index_groups=[order])


def on_device(sliced_state, gate_blocks, gate_slot, samples):
    shape = jax.ShapeDtypeStruct
    state = sliced_state.reshape(Z, 2, X, 32, W)
    packed, slots = pl.pallas_call(
        pack_kernel,
        out_shape=(shape((Z * X, 40, W), BF), shape((1, Z * X), I32)),
        in_specs=[HB, HB, HB],
        out_specs=(VM, VM),
        scratch_shapes=[pltpu.VMEM((Z, 2, X, 32, W), BF), pltpu.VMEM((X, 8, W), BF), pltpu.SemaphoreType.DMA((Z + 2,))],
        compiler_params=CP,
        name="pack",
    )(hbm(state), hbm(gate_blocks.reshape(X, M, 8, W)), hbm(gate_slot.reshape(1, Z * X)))
    packed = exchange(packed, ("z", "x"), ZX_ORDER)
    plane = pl.pallas_call(
        sum_kernel,
        out_shape=shape((X * Y, 64, W), BF),
        in_specs=[VM, VM],
        out_specs=VM,
        scratch_shapes=[pltpu.VMEM((32, W), F32)],
        compiler_params=CP, name="sum",
    )(slots, packed)
    plane = exchange(plane, ("x", "y"), XY_ORDER)
    pair = lax.ppermute(plane, "k", [(0, 1), (1, 0)])
    hot = pl.pallas_call(
        hot_kernel,
        out_shape=shape((2 * W, 4096), BF),
        in_specs=[VM, ANY],
        out_specs=VM,
        compiler_params=CP,
        cost_estimate=pl.CostEstimate(flops=2**22, bytes_accessed=2**21, transcendentals=0),
        name="hot",
    )(samples, plane)
    amplitudes, picked = pl.pallas_call(
        apply_kernel,
        out_shape=(shape((1, 16, 2, W), F32), shape((Z, 40, W), BF)),
        in_specs=[VM, VM, VM, VM],
        out_specs=(VM, VM),
        scratch_shapes=[pltpu.VMEM((X * Y, K, 64, W), BF), pltpu.VMEM((X, 2, W, W), F32), pltpu.VMEM((32, W), F32)],
        compiler_params=CP, name="apply",
    )(samples, hot, plane, pair)
    picked = exchange(picked, "z", Z_ORDER)
    probs, score, amplitudes = pl.pallas_call(
        finish_kernel,
        out_shape=(shape((Z, 4096), F32), shape((1, Z), F32), shape((1, 16, 2, W), F32)),
        in_specs=[VM, VM],
        out_specs=(VM, VM, VM),
        scratch_shapes=[pltpu.VMEM((Z * 32, W), F32)],
        compiler_params=CP, name="finish",
    )(picked, amplitudes)
    return amplitudes, probs, score.reshape(Z)


def solution(mesh):
    split = Mesh(mesh.devices.reshape(Z, X, Y, K), ("z", "x", "y", "k"))
    placed = (P(None, ("z", "x"), None, ("y", "k"), None, None), P(("z", "x"), None, None, None), P(), P())
    return jax.shard_map(
        on_device,
        mesh=split,
        in_specs=placed,
        out_specs=(P(("z", "x"), ("y", "k"), None, None), P(), P()),
        check_vma=False,
    )
```

```python
import functools

import jax
import jax.numpy as jnp
from jax import lax
from jax.experimental import pallas as pl
from jax.experimental.pallas import tpu as pltpu
from jax.sharding import Mesh
from jax.sharding import PartitionSpec as P

BF, F32, I32 = jnp.bfloat16, jnp.float32, jnp.int32
Z, X, Y, K = 8, 4, 4, 2
M = Y * K
W = 128
Z_FIRST, X_FIRST, Y_FIRST = 4, 2, 2
CP = pltpu.CompilerParams(vmem_limit_bytes=8 * 2**20)
VM = pl.BlockSpec(memory_space=pltpu.VMEM)
ANY = pl.BlockSpec(memory_space=pl.ANY)
HB = pl.BlockSpec(memory_space=pltpu.HBM)


def led_by(first, count):
    return [first] + [i for i in range(count) if i != first]


Z_ORDER, X_ORDER, Y_ORDER = led_by(Z_FIRST, Z), led_by(X_FIRST, X), led_by(Y_FIRST, Y)
ZX_ORDER = [z * X + x for z in Z_ORDER for x in X_ORDER]
XY_ORDER = [x * Y + y for y in Y_ORDER for x in X_ORDER]


def mode_index():
    return lax.axis_index("y") * K + lax.axis_index("k")


def dot(a, b):
    return jnp.dot(a, b, preferred_element_type=F32)


def pack_kernel(state_ref, gates_ref, slot_ref, out_ref, slot_out_ref, held_ref, rows_ref, sems):
    copies = [pltpu.make_async_copy(state_ref.at[c], held_ref.at[c], sems.at[c]) for c in range(Z)]
    for copy in copies:
        copy.start()
    rows = pltpu.make_async_copy(gates_ref.at[:, mode_index()], rows_ref, sems.at[Z])
    rows.start()
    slots = pltpu.make_async_copy(slot_ref, slot_out_ref, sems.at[Z + 1])
    slots.start()
    for c in range(Z):
        copies[c].wait()
        for s in range(X):
            total = held_ref[c, 0, s].astype(F32) + held_ref[c, 1, s].astype(F32)
            out_ref[ZX_ORDER.index(c * X + s), 0:32, :] = total.astype(BF)
    rows.wait()
    slots.wait()
    for s in range(X):
        for c in range(Z):
            out_ref[ZX_ORDER.index(c * X + s), 32:40, :] = rows_ref[s]


def sum_kernel(slot_ref, in_ref, out_ref, sum_ref):
    first = lax.axis_index("z") * 4
    slots = jnp.broadcast_to(slot_ref[...], (8, Z * X))
    blocks = lax.broadcasted_iota(I32, (8, Z * X), 1) - first
    wanted = [jnp.sum(jnp.where(blocks == b, slots, 0), axis=1, keepdims=True) for b in range(4)]
    total = jnp.zeros((32, W), F32)
    gates = [jnp.zeros((8, W), F32) for _ in range(4)]
    for i, owner in enumerate(ZX_ORDER):
        total = total + in_ref[i, 0:32, :].astype(F32)
        rows = in_ref[i, 32:40, :].astype(F32)
        gates = [jnp.where(wanted[b] == owner, rows, gates[b]) for b in range(4)]
    sum_ref[...] = total
    state = jnp.concatenate([sum_ref[pl.ds(0, 16, stride=2), :], sum_ref[pl.ds(1, 16, stride=2), :]], axis=0).astype(BF)
    for i in range(X * Y):
        out_ref[i, 0:32, :] = state
        for b in range(4):
            out_ref[i, 32 + 8 * b : 40 + 8 * b, :] = gates[b].astype(BF)


def embed(real, imag):
    return jnp.concatenate([jnp.concatenate([real, imag], axis=1), jnp.concatenate([-imag, real], axis=1)], axis=0)


def compose(first, second):
    left = jnp.concatenate([first[:W], first[W:]], axis=1)
    return dot(left, embed(second[:W], second[W:]))


def hot_kernel(samples_ref, after_ref, out_ref):
    flat = samples_ref[pl.ds(lax.axis_index("z"), 1), :]
    lane = (((flat >> 14) & 1) * W + (flat & 127)).astype(F32).astype(BF)
    chunk = 512
    ids = lax.broadcasted_iota(I32, (2 * W, chunk), 0).astype(F32).astype(BF)
    for j in range(4096 // chunk):
        hit = ids == lane[:, j * chunk : (j + 1) * chunk]
        out_ref[:, j * chunk : (j + 1) * chunk] = jnp.where(hit, jnp.ones((), BF), jnp.zeros((), BF))


def apply_kernel(samples_ref, hot_ref, own_ref, pair_ref, amp_ref, out_ref, in_ref, full_ref, pick_ref):
    circuit = lax.axis_index("z")
    spect = lax.axis_index("x")
    core = lax.axis_index("k")
    mode = mode_index()
    for i, at in enumerate(XY_ORDER):
        in_ref[at, core] = own_ref[i]
        in_ref[at, 1 - core] = pair_ref[i]
    g = [in_ref[:, :, 32 + 8 * b : 40 + 8 * b, :].reshape(2 * W, W) for b in range(4)]
    col = compose(g[0], g[2]).astype(BF)
    row = compose(g[1], g[3])
    row_r, row_i = row[:, :W].T.astype(BF), row[:, W:].T.astype(BF)
    gate_q = embed(col[:, :W], col[:, W:])
    gate_p = jnp.concatenate([jnp.concatenate([row_r, -row_i], axis=1), jnp.concatenate([row_i, row_r], axis=1)], axis=0)
    real = in_ref[:, :, 0:16, :].reshape(X * W, W)
    imag = in_ref[:, :, 16:32, :].reshape(X * W, W)
    mid = dot(jnp.concatenate([real, imag], axis=1), gate_q).astype(BF)
    mid = jnp.concatenate(
        [jnp.concatenate([mid[s * W : (s + 1) * W, r * W : (r + 1) * W] for s in range(X)], axis=1) for r in range(2)], axis=0
    )
    full = dot(gate_p, mid)
    for s in range(X):
        for r in range(2):
            full_ref[s, r] = full[r * W : (r + 1) * W, s * W : (s + 1) * W]
    start = pl.multiple_of(mode * 16, 16)
    for r in range(2):
        amp_ref[0, :, r, :] = full_ref[spect, r, pl.ds(start, 16), :]
    mag = full[:W] * full[:W] + full[W:] * full[W:]
    norm = jnp.sum(mag)
    table = jnp.concatenate([mag[:, : 2 * W], mag[:, 2 * W :]], axis=0).astype(BF)
    chunk = 512
    ids = lax.broadcasted_iota(I32, (2 * W, chunk), 0).astype(F32).astype(BF)
    for j in range(4096 // chunk):
        flat = samples_ref[pl.ds(circuit, 1), j * chunk : (j + 1) * chunk]
        line = (((flat >> 15) & 1) * W + ((flat >> 7) & 127)).astype(F32).astype(BF)
        got = dot(table, hot_ref[:, j * chunk : (j + 1) * chunk]).astype(BF)
        got = jnp.where(ids == line, got, jnp.zeros((), BF))
        held = got[0:16]
        for i in range(1, 16):
            held = held + got[16 * i : 16 * i + 16]
        got = jnp.sum(held.astype(F32), axis=0, keepdims=True)
        for i in range(chunk // W):
            pick_ref[j * (chunk // W) + i : j * (chunk // W) + i + 1, :] = got[:, i * W : (i + 1) * W]
    picked = pick_ref[...].astype(BF)
    tail = jnp.full((8, W), norm, F32)
    high = tail.astype(BF).astype(F32)
    tail = jnp.where(lax.broadcasted_iota(I32, (8, W), 0) == 0, high, tail - high).astype(BF)
    for c in range(Z):
        out_ref[c, 0:32, :] = picked
        out_ref[c, 32:40, :] = tail


def finish_kernel(in_ref, held_ref, probs_ref, score_ref, amp_ref, wide_ref):
    amp_ref[...] = held_ref[...]
    for i, c in enumerate(Z_ORDER):
        tail = in_ref[i, 32:40, :].astype(F32)
        norm = tail[0:1] + tail[1:2]
        wide_ref[c * 32 : (c + 1) * 32, :] = in_ref[i, 0:32, :].astype(F32) * 65536.0 / norm
    total = jnp.zeros((Z, W), F32)
    for j in range(32):
        rows = wide_ref[pl.ds(j, Z, stride=32), :]
        probs_ref[:, j * W : (j + 1) * W] = rows
        total = total + rows
    score = jnp.sum(total, axis=1, keepdims=True) * (1.0 / 4096.0)
    diag = lax.broadcasted_iota(I32, (Z, W), 0) == lax.broadcasted_iota(I32, (Z, W), 1)
    score_ref[...] = jnp.sum(jnp.where(diag, score, 0.0), axis=0, keepdims=True)[:, :Z]


def hbm(array):
    return pltpu.with_memory_space_constraint(array, pltpu.HBM)


def exchange(array, axes, order):
    return lax.all_to_all(array, axes, split_axis=0, concat_axis=0, tiled=True, axis_index_groups=[order])


def on_device(sliced_state, gate_blocks, gate_slot, samples):
    shape = jax.ShapeDtypeStruct
    state = sliced_state.reshape(Z, 2, X, 32, W)
    packed, slots = pl.pallas_call(
        pack_kernel,
        out_shape=(shape((Z * X, 40, W), BF), shape((1, Z * X), I32)),
        in_specs=[HB, HB, HB],
        out_specs=(VM, VM),
        scratch_shapes=[pltpu.VMEM((Z, 2, X, 32, W), BF), pltpu.VMEM((X, 8, W), BF), pltpu.SemaphoreType.DMA((Z + 2,))],
        compiler_params=CP,
        name="pack",
    )(hbm(state), hbm(gate_blocks.reshape(X, M, 8, W)), hbm(gate_slot.reshape(1, Z * X)))
    packed = exchange(packed, ("z", "x"), ZX_ORDER)
    plane = pl.pallas_call(
        sum_kernel,
        out_shape=shape((X * Y, 64, W), BF),
        in_specs=[VM, VM],
        out_specs=VM,
        scratch_shapes=[pltpu.VMEM((32, W), F32)],
        compiler_params=CP, name="sum",
    )(slots, packed)
    plane = exchange(plane, ("x", "y"), XY_ORDER)
    pair = lax.ppermute(plane, "k", [(0, 1), (1, 0)])
    hot = pl.pallas_call(
        hot_kernel,
        out_shape=shape((2 * W, 4096), BF),
        in_specs=[VM, ANY],
        out_specs=VM,
        compiler_params=CP,
        cost_estimate=pl.CostEstimate(flops=2**22, bytes_accessed=2**21, transcendentals=0),
        name="hot",
    )(samples, plane)
    amplitudes, picked = pl.pallas_call(
        apply_kernel,
        out_shape=(shape((1, 16, 2, W), F32), shape((Z, 40, W), BF)),
        in_specs=[VM, VM, VM, VM],
        out_specs=(VM, VM),
        scratch_shapes=[pltpu.VMEM((X * Y, K, 64, W), BF), pltpu.VMEM((X, 2, W, W), F32), pltpu.VMEM((32, W), F32)],
        compiler_params=CP, name="apply",
    )(samples, hot, plane, pair)
    picked = exchange(picked, "z", Z_ORDER)
    probs, score, amplitudes = pl.pallas_call(
        finish_kernel,
        out_shape=(shape((Z, 4096), F32), shape((1, Z), F32), shape((1, 16, 2, W), F32)),
        in_specs=[VM, VM],
        out_specs=(VM, VM, VM),
        scratch_shapes=[pltpu.VMEM((Z * 32, W), F32)],
        compiler_params=CP, name="finish",
    )(picked, amplitudes)
    return amplitudes, probs, score.reshape(Z)


def solution(mesh):
    split = Mesh(mesh.devices.reshape(Z, X, Y, K), ("z", "x", "y", "k"))
    placed = (P(None, ("z", "x"), None, ("y", "k"), None, None), P(("z", "x"), None, None, None), P(), P())
    return jax.shard_map(
        on_device,
        mesh=split,
        in_specs=placed,
        out_specs=(P(("z", "x"), ("y", "k"), None, None), P(), P()),
        check_vma=False,
    )
```

```python
import functools

import jax
import jax.numpy as jnp
from jax import lax
from jax.experimental import pallas as pl
from jax.experimental.pallas import tpu as pltpu
from jax.sharding import Mesh
from jax.sharding import PartitionSpec as P

BF, F32, I32 = jnp.bfloat16, jnp.float32, jnp.int32
Z, X, Y, K = 8, 4, 4, 2
M = Y * K
W = 128
Z_FIRST, X_FIRST, Y_FIRST = 4, 2, 2
CP = pltpu.CompilerParams(vmem_limit_bytes=8 * 2**20)
VM = pl.BlockSpec(memory_space=pltpu.VMEM)
ANY = pl.BlockSpec(memory_space=pl.ANY)
HB = pl.BlockSpec(memory_space=pltpu.HBM)


def led_by(first, count):
    return [first] + [i for i in range(count) if i != first]


Z_ORDER, X_ORDER, Y_ORDER = led_by(Z_FIRST, Z), led_by(X_FIRST, X), led_by(Y_FIRST, Y)
ZX_ORDER = [z * X + x for z in Z_ORDER for x in X_ORDER]
XY_ORDER = [x * Y + y for y in Y_ORDER for x in X_ORDER]


def mode_index():
    return lax.axis_index("y") * K + lax.axis_index("k")


def dot(a, b):
    return jnp.dot(a, b, preferred_element_type=F32)


def pack_kernel(state_ref, gates_ref, slot_ref, out_ref, slot_out_ref, held_ref, rows_ref, sems):
    copies = [pltpu.make_async_copy(state_ref.at[c, i], held_ref.at[c, i], sems.at[2 * c + i]) for c in range(Z) for i in range(2)]
    for copy in copies:
        copy.start()
    rows = pltpu.make_async_copy(gates_ref.at[:, mode_index()], rows_ref, sems.at[2 * Z])
    rows.start()
    slots = pltpu.make_async_copy(slot_ref, slot_out_ref, sems.at[2 * Z + 1])
    slots.start()
    for c in range(Z):
        copies[2 * c].wait()
        copies[2 * c + 1].wait()
        for s in range(X):
            total = held_ref[c, 0, s].astype(F32) + held_ref[c, 1, s].astype(F32)
            out_ref[ZX_ORDER.index(c * X + s), 0:32, :] = total.astype(BF)
    rows.wait()
    slots.wait()
    for s in range(X):
        for c in range(Z):
            out_ref[ZX_ORDER.index(c * X + s), 32:40, :] = rows_ref[s]


def sum_kernel(slot_ref, in_ref, out_ref, sum_ref):
    first = lax.axis_index("z") * 4
    slots = jnp.broadcast_to(slot_ref[...], (8, Z * X))
    blocks = lax.broadcasted_iota(I32, (8, Z * X), 1) - first
    wanted = [jnp.sum(jnp.where(blocks == b, slots, 0), axis=1, keepdims=True) for b in range(4)]
    total = jnp.zeros((32, W), F32)
    gates = [jnp.zeros((8, W), F32) for _ in range(4)]
    for i, owner in enumerate(ZX_ORDER):
        total = total + in_ref[i, 0:32, :].astype(F32)
        rows = in_ref[i, 32:40, :].astype(F32)
        gates = [jnp.where(wanted[b] == owner, rows, gates[b]) for b in range(4)]
    sum_ref[...] = total
    state = jnp.concatenate([sum_ref[pl.ds(0, 16, stride=2), :], sum_ref[pl.ds(1, 16, stride=2), :]], axis=0).astype(BF)
    for i in range(X * Y):
        out_ref[i, 0:32, :] = state
        for b in range(4):
            out_ref[i, 32 + 8 * b : 40 + 8 * b, :] = gates[b].astype(BF)


def embed(real, imag):
    return jnp.concatenate([jnp.concatenate([real, imag], axis=1), jnp.concatenate([-imag, real], axis=1)], axis=0)


def compose(first, second):
    left = jnp.concatenate([first[:W], first[W:]], axis=1)
    return dot(left, embed(second[:W], second[W:]))


def hot_kernel(samples_ref, after_ref, out_ref):
    flat = samples_ref[pl.ds(lax.axis_index("z"), 1), :]
    lane = (((flat >> 14) & 1) * W + (flat & 127)).astype(F32).astype(BF)
    chunk = 512
    ids = lax.broadcasted_iota(I32, (2 * W, chunk), 0).astype(F32).astype(BF)
    for j in range(4096 // chunk):
        hit = ids == lane[:, j * chunk : (j + 1) * chunk]
        out_ref[:, j * chunk : (j + 1) * chunk] = jnp.where(hit, jnp.ones((), BF), jnp.zeros((), BF))


def apply_kernel(samples_ref, hot_ref, own_ref, pair_ref, amp_ref, out_ref, in_ref, full_ref, pick_ref):
    circuit = lax.axis_index("z")
    spect = lax.axis_index("x")
    core = lax.axis_index("k")
    mode = mode_index()
    for i, at in enumerate(XY_ORDER):
        in_ref[at, core] = own_ref[i]
        in_ref[at, 1 - core] = pair_ref[i]
    g = [in_ref[:, :, 32 + 8 * b : 40 + 8 * b, :].reshape(2 * W, W) for b in range(4)]
    col = compose(g[0], g[2]).astype(BF)
    row = compose(g[1], g[3])
    row_r, row_i = row[:, :W].T.astype(BF), row[:, W:].T.astype(BF)
    gate_q = embed(col[:, :W], col[:, W:])
    gate_p = jnp.concatenate([jnp.concatenate([row_r, -row_i], axis=1), jnp.concatenate([row_i, row_r], axis=1)], axis=0)
    real = in_ref[:, :, 0:16, :].reshape(X * W, W)
    imag = in_ref[:, :, 16:32, :].reshape(X * W, W)
    mid = dot(jnp.concatenate([real, imag], axis=1), gate_q).astype(BF)
    mid = jnp.concatenate(
        [jnp.concatenate([mid[s * W : (s + 1) * W, r * W : (r + 1) * W] for s in range(X)], axis=1) for r in range(2)], axis=0
    )
    full = dot(gate_p, mid)
    for s in range(X):
        for r in range(2):
            full_ref[s, r] = full[r * W : (r + 1) * W, s * W : (s + 1) * W]
    start = pl.multiple_of(mode * 16, 16)
    for r in range(2):
        amp_ref[0, :, r, :] = full_ref[spect, r, pl.ds(start, 16), :]
    mag = full[:W] * full[:W] + full[W:] * full[W:]
    norm = jnp.sum(mag)
    table = jnp.concatenate([mag[:, : 2 * W], mag[:, 2 * W :]], axis=0).astype(BF)
    chunk = 512
    ids = lax.broadcasted_iota(I32, (2 * W, chunk), 0).astype(F32).astype(BF)
    for j in range(4096 // chunk):
        flat = samples_ref[pl.ds(circuit, 1), j * chunk : (j + 1) * chunk]
        line = (((flat >> 15) & 1) * W + ((flat >> 7) & 127)).astype(F32).astype(BF)
        got = dot(table, hot_ref[:, j * chunk : (j + 1) * chunk]).astype(BF)
        got = jnp.where(ids == line, got, jnp.zeros((), BF))
        held = got[0:16]
        for i in range(1, 16):
            held = held + got[16 * i : 16 * i + 16]
        got = jnp.sum(held.astype(F32), axis=0, keepdims=True)
        for i in range(chunk // W):
            pick_ref[j * (chunk // W) + i : j * (chunk // W) + i + 1, :] = got[:, i * W : (i + 1) * W]
    picked = pick_ref[...].astype(BF)
    tail = jnp.full((8, W), norm, F32)
    high = tail.astype(BF).astype(F32)
    tail = jnp.where(lax.broadcasted_iota(I32, (8, W), 0) == 0, high, tail - high).astype(BF)
    for c in range(Z):
        out_ref[c, 0:32, :] = picked
        out_ref[c, 32:40, :] = tail


def finish_kernel(in_ref, held_ref, probs_ref, score_ref, amp_ref, wide_ref, done_ref, mean_ref, sems):
    amps = pltpu.make_async_copy(held_ref, amp_ref, sems.at[4])
    amps.start()
    for i, c in enumerate(Z_ORDER):
        tail = in_ref[i, 32:40, :].astype(F32)
        norm = tail[0:1] + tail[1:2]
        wide_ref[c * 32 : (c + 1) * 32, :] = in_ref[i, 0:32, :].astype(F32) * 65536.0 / norm
    total = jnp.zeros((Z, W), F32)
    copies = []
    for part in range(4):
        for j in range(8 * part, 8 * part + 8):
            rows = wide_ref[pl.ds(j, Z, stride=32), :]
            done_ref[:, j * W : (j + 1) * W] = rows
            total = total + rows
        lanes = pl.ds(part * 1024, 1024)
        copies.append(pltpu.make_async_copy(done_ref.at[:, lanes], probs_ref.at[:, lanes], sems.at[part]))
        copies[-1].start()
    score = jnp.sum(total, axis=1, keepdims=True) * (1.0 / 4096.0)
    diag = lax.broadcasted_iota(I32, (Z, W), 0) == lax.broadcasted_iota(I32, (Z, W), 1)
    mean_ref[...] = jnp.sum(jnp.where(diag, score, 0.0), axis=0, keepdims=True)[:, :Z]
    copies.append(pltpu.make_async_copy(mean_ref, score_ref, sems.at[5]))
    copies[-1].start()
    for copy in copies:
        copy.wait()
    amps.wait()


def hbm(array):
    return pltpu.with_memory_space_constraint(array, pltpu.HBM)


def exchange(array, axes, order):
    return lax.all_to_all(array, axes, split_axis=0, concat_axis=0, tiled=True, axis_index_groups=[order])


def on_device(sliced_state, gate_blocks, gate_slot, samples):
    shape = jax.ShapeDtypeStruct
    state = sliced_state.reshape(Z, 2, X, 32, W)
    packed, slots = pl.pallas_call(
        pack_kernel,
        out_shape=(shape((Z * X, 40, W), BF), shape((1, Z * X), I32)),
        in_specs=[HB, HB, HB],
        out_specs=(VM, VM),
        scratch_shapes=[pltpu.VMEM((Z, 2, X, 32, W), BF), pltpu.VMEM((X, 8, W), BF), pltpu.SemaphoreType.DMA((2 * Z + 2,))],
        compiler_params=CP,
        name="pack",
    )(hbm(state), hbm(gate_blocks.reshape(X, M, 8, W)), hbm(gate_slot.reshape(1, Z * X)))
    packed = exchange(packed, ("z", "x"), ZX_ORDER)
    plane = pl.pallas_call(
        sum_kernel,
        out_shape=shape((X * Y, 64, W), BF),
        in_specs=[VM, VM],
        out_specs=VM,
        scratch_shapes=[pltpu.VMEM((32, W), F32)],
        compiler_params=CP, name="sum",
    )(slots, packed)
    plane = exchange(plane, ("x", "y"), XY_ORDER)
    pair = lax.ppermute(plane, "k", [(0, 1), (1, 0)])
    hot = pl.pallas_call(
        hot_kernel,
        out_shape=shape((2 * W, 4096), BF),
        in_specs=[VM, ANY],
        out_specs=VM,
        compiler_params=CP,
        cost_estimate=pl.CostEstimate(flops=2**22, bytes_accessed=2**21, transcendentals=0),
        name="hot",
    )(samples, plane)
    amplitudes, picked = pl.pallas_call(
        apply_kernel,
        out_shape=(shape((1, 16, 2, W), F32), shape((Z, 40, W), BF)),
        in_specs=[VM, VM, VM, VM],
        out_specs=(VM, VM),
        scratch_shapes=[pltpu.VMEM((X * Y, K, 64, W), BF), pltpu.VMEM((X, 2, W, W), F32), pltpu.VMEM((32, W), F32)],
        compiler_params=CP, name="apply",
    )(samples, hot, plane, pair)
    picked = exchange(picked, "z", Z_ORDER)
    probs, score, amplitudes = pl.pallas_call(
        finish_kernel,
        out_shape=(shape((Z, 4096), F32), shape((1, Z), F32), shape((1, 16, 2, W), F32)),
        in_specs=[VM, VM],
        out_specs=(ANY, ANY, ANY),
        scratch_shapes=[pltpu.VMEM((Z * 32, W), F32), pltpu.VMEM((Z, 4096), F32), pltpu.VMEM((1, Z), F32), pltpu.SemaphoreType.DMA((6,))],
        compiler_params=CP, name="finish",
    )(picked, amplitudes)
    return amplitudes, probs, score.reshape(Z)


def solution(mesh):
    split = Mesh(mesh.devices.reshape(Z, X, Y, K), ("z", "x", "y", "k"))
    placed = (P(None, ("z", "x"), None, ("y", "k"), None, None), P(("z", "x"), None, None, None), P(), P())
    return jax.shard_map(
        on_device,
        mesh=split,
        in_specs=placed,
        out_specs=(P(("z", "x"), ("y", "k"), None, None), P(), P()),
        check_vma=False,
    )
```

```python
import functools

import jax
import jax.numpy as jnp
from jax import lax
from jax.experimental import pallas as pl
from jax.experimental.pallas import tpu as pltpu
from jax.sharding import Mesh
from jax.sharding import PartitionSpec as P

BF, F32, I32 = jnp.bfloat16, jnp.float32, jnp.int32
Z, X, Y, K = 8, 4, 4, 2
M = Y * K
W = 128
Z_FIRST, X_FIRST, Y_FIRST = 4, 2, 2
CP = pltpu.CompilerParams(vmem_limit_bytes=8 * 2**20)
VM = pl.BlockSpec(memory_space=pltpu.VMEM)
ANY = pl.BlockSpec(memory_space=pl.ANY)
HB = pl.BlockSpec(memory_space=pltpu.HBM)


def led_by(first, count):
    return [first] + [i for i in range(count) if i != first]


Z_LAST = [4, 0, 7, 1, 6, 2, 5, 3]
Z_ORDER, X_ORDER, Y_ORDER = led_by(Z_FIRST, Z), led_by(X_FIRST, X), led_by(Y_FIRST, Y)
ZX_ORDER = [z * X + x for z in Z_ORDER for x in X_ORDER]
XY_ORDER = [x * Y + y for y in Y_ORDER for x in X_ORDER]


def mode_index():
    return lax.axis_index("y") * K + lax.axis_index("k")


def dot(a, b):
    return jnp.dot(a, b, preferred_element_type=F32)


def pack_kernel(state_ref, gates_ref, slot_ref, out_ref, slot_out_ref, held_ref, rows_ref, sems):
    copies = [pltpu.make_async_copy(state_ref.at[c, i], held_ref.at[c, i], sems.at[2 * c + i]) for c in range(Z) for i in range(2)]
    for copy in copies:
        copy.start()
    rows = pltpu.make_async_copy(gates_ref.at[:, mode_index()], rows_ref, sems.at[2 * Z])
    rows.start()
    slots = pltpu.make_async_copy(slot_ref, slot_out_ref, sems.at[2 * Z + 1])
    slots.start()
    for c in range(Z):
        copies[2 * c].wait()
        copies[2 * c + 1].wait()
        for s in range(X):
            total = held_ref[c, 0, s].astype(F32) + held_ref[c, 1, s].astype(F32)
            out_ref[ZX_ORDER.index(c * X + s), 0:32, :] = total.astype(BF)
    rows.wait()
    slots.wait()
    for s in range(X):
        for c in range(Z):
            out_ref[ZX_ORDER.index(c * X + s), 32:40, :] = rows_ref[s]


def sum_kernel(slot_ref, in_ref, out_ref, sum_ref):
    first = lax.axis_index("z") * 4
    slots = jnp.broadcast_to(slot_ref[...], (8, Z * X))
    blocks = lax.broadcasted_iota(I32, (8, Z * X), 1) - first
    wanted = [jnp.sum(jnp.where(blocks == b, slots, 0), axis=1, keepdims=True) for b in range(4)]
    total = jnp.zeros((32, W), F32)
    gates = [jnp.zeros((8, W), F32) for _ in range(4)]
    for i, owner in enumerate(ZX_ORDER):
        total = total + in_ref[i, 0:32, :].astype(F32)
        rows = in_ref[i, 32:40, :].astype(F32)
        gates = [jnp.where(wanted[b] == owner, rows, gates[b]) for b in range(4)]
    sum_ref[...] = total
    state = jnp.concatenate([sum_ref[pl.ds(0, 16, stride=2), :], sum_ref[pl.ds(1, 16, stride=2), :]], axis=0).astype(BF)
    for i in range(X * Y):
        out_ref[i, 0:32, :] = state
        for b in range(4):
            out_ref[i, 32 + 8 * b : 40 + 8 * b, :] = gates[b].astype(BF)


def embed(real, imag):
    return jnp.concatenate([jnp.concatenate([real, imag], axis=1), jnp.concatenate([-imag, real], axis=1)], axis=0)


def compose(first, second):
    left = jnp.concatenate([first[:W], first[W:]], axis=1)
    return dot(left, embed(second[:W], second[W:]))


def hot_kernel(samples_ref, after_ref, out_ref):
    flat = samples_ref[pl.ds(lax.axis_index("z"), 1), :]
    lane = (((flat >> 14) & 1) * W + (flat & 127)).astype(F32).astype(BF)
    chunk = 512
    ids = lax.broadcasted_iota(I32, (2 * W, chunk), 0).astype(F32).astype(BF)
    for j in range(4096 // chunk):
        hit = ids == lane[:, j * chunk : (j + 1) * chunk]
        out_ref[:, j * chunk : (j + 1) * chunk] = jnp.where(hit, jnp.ones((), BF), jnp.zeros((), BF))


def apply_kernel(samples_ref, hot_ref, own_ref, pair_ref, amp_ref, out_ref, in_ref, full_ref, pick_ref):
    circuit = lax.axis_index("z")
    spect = lax.axis_index("x")
    core = lax.axis_index("k")
    mode = mode_index()
    for i, at in enumerate(XY_ORDER):
        in_ref[at, core] = own_ref[i]
        in_ref[at, 1 - core] = pair_ref[i]
    g = [in_ref[:, :, 32 + 8 * b : 40 + 8 * b, :].reshape(2 * W, W) for b in range(4)]
    col = compose(g[0], g[2]).astype(BF)
    row = compose(g[1], g[3])
    row_r, row_i = row[:, :W].T.astype(BF), row[:, W:].T.astype(BF)
    gate_q = embed(col[:, :W], col[:, W:])
    gate_p = jnp.concatenate([jnp.concatenate([row_r, -row_i], axis=1), jnp.concatenate([row_i, row_r], axis=1)], axis=0)
    real = in_ref[:, :, 0:16, :].reshape(X * W, W)
    imag = in_ref[:, :, 16:32, :].reshape(X * W, W)
    mid = dot(jnp.concatenate([real, imag], axis=1), gate_q).astype(BF)
    mid = jnp.concatenate(
        [jnp.concatenate([mid[s * W : (s + 1) * W, r * W : (r + 1) * W] for s in range(X)], axis=1) for r in range(2)], axis=0
    )
    full = dot(gate_p, mid)
    for s in range(X):
        for r in range(2):
            full_ref[s, r] = full[r * W : (r + 1) * W, s * W : (s + 1) * W]
    start = pl.multiple_of(mode * 16, 16)
    for r in range(2):
        amp_ref[0, :, r, :] = full_ref[spect, r, pl.ds(start, 16), :]
    mag = full[:W] * full[:W] + full[W:] * full[W:]
    norm = jnp.sum(mag)
    table = jnp.concatenate([mag[:, : 2 * W], mag[:, 2 * W :]], axis=0).astype(BF)
    chunk = 512
    ids = lax.broadcasted_iota(I32, (2 * W, chunk), 0).astype(F32).astype(BF)
    for j in range(4096 // chunk):
        flat = samples_ref[pl.ds(circuit, 1), j * chunk : (j + 1) * chunk]
        line = (((flat >> 15) & 1) * W + ((flat >> 7) & 127)).astype(F32).astype(BF)
        got = dot(table, hot_ref[:, j * chunk : (j + 1) * chunk]).astype(BF)
        got = jnp.where(ids == line, got, jnp.zeros((), BF))
        held = got[0:16]
        for i in range(1, 16):
            held = held + got[16 * i : 16 * i + 16]
        got = jnp.sum(held.astype(F32), axis=0, keepdims=True)
        for i in range(chunk // W):
            pick_ref[j * (chunk // W) + i : j * (chunk // W) + i + 1, :] = got[:, i * W : (i + 1) * W]
    picked = pick_ref[...].astype(BF)
    tail = jnp.full((8, W), norm, F32)
    high = tail.astype(BF).astype(F32)
    tail = jnp.where(lax.broadcasted_iota(I32, (8, W), 0) == 0, high, tail - high).astype(BF)
    for c in range(Z):
        out_ref[c, 0:32, :] = picked
        out_ref[c, 32:40, :] = tail


def finish_kernel(in_ref, held_ref, probs_ref, score_ref, amp_ref, wide_ref, done_ref, mean_ref, sems):
    amps = pltpu.make_async_copy(held_ref, amp_ref, sems.at[4])
    amps.start()
    for i, c in enumerate(Z_LAST):
        tail = in_ref[i, 32:40, :].astype(F32)
        norm = tail[0:1] + tail[1:2]
        wide_ref[c * 32 : (c + 1) * 32, :] = in_ref[i, 0:32, :].astype(F32) * 65536.0 / norm
    total = jnp.zeros((Z, W), F32)
    copies = []
    for part in range(4):
        for j in range(8 * part, 8 * part + 8):
            rows = wide_ref[pl.ds(j, Z, stride=32), :]
            done_ref[:, j * W : (j + 1) * W] = rows
            total = total + rows
        lanes = pl.ds(part * 1024, 1024)
        copies.append(pltpu.make_async_copy(done_ref.at[:, lanes], probs_ref.at[:, lanes], sems.at[part]))
        copies[-1].start()
    score = jnp.sum(total, axis=1, keepdims=True) * (1.0 / 4096.0)
    diag = lax.broadcasted_iota(I32, (Z, W), 0) == lax.broadcasted_iota(I32, (Z, W), 1)
    mean_ref[...] = jnp.sum(jnp.where(diag, score, 0.0), axis=0, keepdims=True)[:, :Z]
    copies.append(pltpu.make_async_copy(mean_ref, score_ref, sems.at[5]))
    copies[-1].start()
    for copy in copies:
        copy.wait()
    amps.wait()


def hbm(array):
    return pltpu.with_memory_space_constraint(array, pltpu.HBM)


def exchange(array, axes, order):
    return lax.all_to_all(array, axes, split_axis=0, concat_axis=0, tiled=True, axis_index_groups=[order])


def on_device(sliced_state, gate_blocks, gate_slot, samples):
    shape = jax.ShapeDtypeStruct
    state = sliced_state.reshape(Z, 2, X, 32, W)
    packed, slots = pl.pallas_call(
        pack_kernel,
        out_shape=(shape((Z * X, 40, W), BF), shape((1, Z * X), I32)),
        in_specs=[HB, HB, HB],
        out_specs=(VM, VM),
        scratch_shapes=[pltpu.VMEM((Z, 2, X, 32, W), BF), pltpu.VMEM((X, 8, W), BF), pltpu.SemaphoreType.DMA((2 * Z + 2,))],
        compiler_params=CP,
        name="pack",
    )(hbm(state), hbm(gate_blocks.reshape(X, M, 8, W)), hbm(gate_slot.reshape(1, Z * X)))
    packed = exchange(packed, ("z", "x"), ZX_ORDER)
    plane = pl.pallas_call(
        sum_kernel,
        out_shape=shape((X * Y, 64, W), BF),
        in_specs=[VM, VM],
        out_specs=VM,
        scratch_shapes=[pltpu.VMEM((32, W), F32)],
        compiler_params=CP, name="sum",
    )(slots, packed)
    plane = exchange(plane, ("x", "y"), XY_ORDER)
    pair = lax.ppermute(plane, "k", [(0, 1), (1, 0)])
    hot = pl.pallas_call(
        hot_kernel,
        out_shape=shape((2 * W, 4096), BF),
        in_specs=[VM, ANY],
        out_specs=VM,
        compiler_params=CP,
        cost_estimate=pl.CostEstimate(flops=2**22, bytes_accessed=2**21, transcendentals=0),
        name="hot",
    )(samples, plane)
    amplitudes, picked = pl.pallas_call(
        apply_kernel,
        out_shape=(shape((1, 16, 2, W), F32), shape((Z, 40, W), BF)),
        in_specs=[VM, VM, VM, VM],
        out_specs=(VM, VM),
        scratch_shapes=[pltpu.VMEM((X * Y, K, 64, W), BF), pltpu.VMEM((X, 2, W, W), F32), pltpu.VMEM((32, W), F32)],
        compiler_params=CP, name="apply",
    )(samples, hot, plane, pair)
    picked = exchange(picked, "z", Z_LAST)
    probs, score, amplitudes = pl.pallas_call(
        finish_kernel,
        out_shape=(shape((Z, 4096), F32), shape((1, Z), F32), shape((1, 16, 2, W), F32)),
        in_specs=[VM, VM],
        out_specs=(ANY, ANY, ANY),
        scratch_shapes=[pltpu.VMEM((Z * 32, W), F32), pltpu.VMEM((Z, 4096), F32), pltpu.VMEM((1, Z), F32), pltpu.SemaphoreType.DMA((6,))],
        compiler_params=CP, name="finish",
    )(picked, amplitudes)
    return amplitudes, probs, score.reshape(Z)


def solution(mesh):
    split = Mesh(mesh.devices.reshape(Z, X, Y, K), ("z", "x", "y", "k"))
    placed = (P(None, ("z", "x"), None, ("y", "k"), None, None), P(("z", "x"), None, None, None), P(), P())
    return jax.shard_map(
        on_device,
        mesh=split,
        in_specs=placed,
        out_specs=(P(("z", "x"), ("y", "k"), None, None), P(), P()),
        check_vma=False,
    )
```

```python
import functools

import jax
import jax.numpy as jnp
from jax import lax
from jax.experimental import pallas as pl
from jax.experimental.pallas import tpu as pltpu
from jax.sharding import Mesh
from jax.sharding import PartitionSpec as P

BF, F32, I32 = jnp.bfloat16, jnp.float32, jnp.int32
Z, X, Y, K = 8, 4, 4, 2
M = Y * K
W = 128
Z_FIRST, X_FIRST, Y_FIRST = 4, 2, 2
CP = pltpu.CompilerParams(vmem_limit_bytes=8 * 2**20)
VM = pl.BlockSpec(memory_space=pltpu.VMEM)
ANY = pl.BlockSpec(memory_space=pl.ANY)
HB = pl.BlockSpec(memory_space=pltpu.HBM)


def led_by(first, count):
    return [first] + [i for i in range(count) if i != first]


Z_ORDER, X_ORDER, Y_ORDER = led_by(Z_FIRST, Z), led_by(X_FIRST, X), led_by(Y_FIRST, Y)
ZX_ORDER = [z * X + x for z in Z_ORDER for x in X_ORDER]
XY_ORDER = [x * Y + y for y in Y_ORDER for x in X_ORDER]


def mode_index():
    return lax.axis_index("y") * K + lax.axis_index("k")


def dot(a, b):
    return jnp.dot(a, b, preferred_element_type=F32)


def pack_kernel(state_ref, gates_ref, slot_ref, out_ref, slot_out_ref, held_ref, rows_ref, sems):
    copies = [pltpu.make_async_copy(state_ref.at[c, i], held_ref.at[c, i], sems.at[2 * c + i]) for c in range(Z) for i in range(2)]
    for copy in copies:
        copy.start()
    rows = pltpu.make_async_copy(gates_ref.at[:, mode_index()], rows_ref, sems.at[2 * Z])
    rows.start()
    slots = pltpu.make_async_copy(slot_ref, slot_out_ref, sems.at[2 * Z + 1])
    slots.start()
    for c in range(Z):
        copies[2 * c].wait()
        copies[2 * c + 1].wait()
        for s in range(X):
            total = held_ref[c, 0, s].astype(F32) + held_ref[c, 1, s].astype(F32)
            out_ref[ZX_ORDER.index(c * X + s), 0:32, :] = total.astype(BF)
    rows.wait()
    slots.wait()
    for s in range(X):
        for c in range(Z):
            out_ref[ZX_ORDER.index(c * X + s), 32:40, :] = rows_ref[s]


def sum_kernel(slot_ref, in_ref, out_ref, sum_ref):
    first = lax.axis_index("z") * 4
    slots = jnp.broadcast_to(slot_ref[...], (8, Z * X))
    blocks = lax.broadcasted_iota(I32, (8, Z * X), 1) - first
    wanted = [jnp.sum(jnp.where(blocks == b, slots, 0), axis=1, keepdims=True) for b in range(4)]
    total = jnp.zeros((32, W), F32)
    gates = [jnp.zeros((8, W), F32) for _ in range(4)]
    for i, owner in enumerate(ZX_ORDER):
        total = total + in_ref[i, 0:32, :].astype(F32)
        rows = in_ref[i, 32:40, :].astype(F32)
        gates = [jnp.where(wanted[b] == owner, rows, gates[b]) for b in range(4)]
    sum_ref[...] = total
    state = jnp.concatenate([sum_ref[pl.ds(0, 16, stride=2), :], sum_ref[pl.ds(1, 16, stride=2), :]], axis=0).astype(BF)
    for i in range(X * Y):
        out_ref[i, 0:32, :] = state
        for b in range(4):
            out_ref[i, 32 + 8 * b : 40 + 8 * b, :] = gates[b].astype(BF)


def embed(real, imag):
    return jnp.concatenate([jnp.concatenate([real, imag], axis=1), jnp.concatenate([-imag, real], axis=1)], axis=0)


def compose(first, second):
    left = jnp.concatenate([first[:W], first[W:]], axis=1)
    return dot(left, embed(second[:W], second[W:]))


def hot_kernel(samples_ref, after_ref, out_ref):
    flat = samples_ref[pl.ds(lax.axis_index("z"), 1), :]
    lane = (((flat >> 14) & 1) * W + (flat & 127)).astype(F32).astype(BF)
    chunk = 512
    ids = lax.broadcasted_iota(I32, (2 * W, chunk), 0).astype(F32).astype(BF)
    for j in range(4096 // chunk):
        hit = ids == lane[:, j * chunk : (j + 1) * chunk]
        out_ref[:, j * chunk : (j + 1) * chunk] = jnp.where(hit, jnp.ones((), BF), jnp.zeros((), BF))


def apply_kernel(samples_ref, hot_ref, own_ref, pair_ref, amp_ref, out_ref, in_ref, full_ref, pick_ref):
    circuit = lax.axis_index("z")
    spect = lax.axis_index("x")
    core = lax.axis_index("k")
    mode = mode_index()
    for i, at in enumerate(XY_ORDER):
        in_ref[at, core] = own_ref[i]
        in_ref[at, 1 - core] = pair_ref[i]
    g = [in_ref[:, :, 32 + 8 * b : 40 + 8 * b, :].reshape(2 * W, W) for b in range(4)]
    col = compose(g[0], g[2]).astype(BF)
    row = compose(g[1], g[3])
    row_r, row_i = row[:, :W].T.astype(BF), row[:, W:].T.astype(BF)
    gate_q = embed(col[:, :W], col[:, W:])
    gate_p = jnp.concatenate([jnp.concatenate([row_r, -row_i], axis=1), jnp.concatenate([row_i, row_r], axis=1)], axis=0)
    real = in_ref[:, :, 0:16, :].reshape(X * W, W)
    imag = in_ref[:, :, 16:32, :].reshape(X * W, W)
    mid = dot(jnp.concatenate([real, imag], axis=1), gate_q).astype(BF)
    mid = jnp.concatenate(
        [jnp.concatenate([mid[s * W : (s + 1) * W, r * W : (r + 1) * W] for s in range(X)], axis=1) for r in range(2)], axis=0
    )
    full = dot(gate_p, mid)
    for s in range(X):
        for r in range(2):
            full_ref[s, r] = full[r * W : (r + 1) * W, s * W : (s + 1) * W]
    start = pl.multiple_of(mode * 16, 16)
    for r in range(2):
        amp_ref[0, :, r, :] = full_ref[spect, r, pl.ds(start, 16), :]
    mag = full[:W] * full[:W] + full[W:] * full[W:]
    norm = jnp.sum(mag)
    table = jnp.concatenate([mag[:, : 2 * W], mag[:, 2 * W :]], axis=0).astype(BF)
    chunk = 512
    ids = lax.broadcasted_iota(I32, (2 * W, chunk), 0).astype(F32).astype(BF)
    for j in range(4096 // chunk):
        flat = samples_ref[pl.ds(circuit, 1), j * chunk : (j + 1) * chunk]
        line = (((flat >> 15) & 1) * W + ((flat >> 7) & 127)).astype(F32).astype(BF)
        got = dot(table, hot_ref[:, j * chunk : (j + 1) * chunk]).astype(BF)
        got = jnp.where(ids == line, got, jnp.zeros((), BF))
        held = got[0:16]
        for i in range(1, 16):
            held = held + got[16 * i : 16 * i + 16]
        got = jnp.sum(held.astype(F32), axis=0, keepdims=True)
        for i in range(chunk // W):
            pick_ref[j * (chunk // W) + i : j * (chunk // W) + i + 1, :] = got[:, i * W : (i + 1) * W]
    picked = pick_ref[...].astype(BF)
    tail = jnp.full((8, W), norm, F32)
    high = tail.astype(BF).astype(F32)
    tail = jnp.where(lax.broadcasted_iota(I32, (8, W), 0) == 0, high, tail - high).astype(BF)
    for c in range(Z):
        out_ref[c, 0:32, :] = picked
        out_ref[c, 32:40, :] = tail


def finish_kernel(in_ref, held_ref, probs_ref, score_ref, amp_ref, wide_ref):
    amp_ref[...] = held_ref[...]
    for i, c in enumerate(Z_ORDER):
        tail = in_ref[i, 32:40, :].astype(F32)
        norm = tail[0:1] + tail[1:2]
        wide_ref[c * 32 : (c + 1) * 32, :] = in_ref[i, 0:32, :].astype(F32) * 65536.0 / norm
    total = jnp.zeros((Z, W), F32)
    for j in range(32):
        rows = wide_ref[pl.ds(j, Z, stride=32), :]
        probs_ref[:, j * W : (j + 1) * W] = rows
        total = total + rows
    score = jnp.sum(total, axis=1, keepdims=True) * (1.0 / 4096.0)
    diag = lax.broadcasted_iota(I32, (Z, W), 0) == lax.broadcasted_iota(I32, (Z, W), 1)
    score_ref[...] = jnp.sum(jnp.where(diag, score, 0.0), axis=0, keepdims=True)[:, :Z]


def hbm(array):
    return pltpu.with_memory_space_constraint(array, pltpu.HBM)


def exchange(array, axes, order):
    return lax.all_to_all(array, axes, split_axis=0, concat_axis=0, tiled=True, axis_index_groups=[order])


def on_device(sliced_state, gate_blocks, gate_slot, samples):
    shape = jax.ShapeDtypeStruct
    state = sliced_state.reshape(Z, 2, X, 32, W)
    packed, slots = pl.pallas_call(
        pack_kernel,
        out_shape=(shape((Z * X, 40, W), BF), shape((1, Z * X), I32)),
        in_specs=[HB, HB, HB],
        out_specs=(VM, VM),
        scratch_shapes=[pltpu.VMEM((Z, 2, X, 32, W), BF), pltpu.VMEM((X, 8, W), BF), pltpu.SemaphoreType.DMA((2 * Z + 2,))],
        compiler_params=CP,
        name="pack",
    )(hbm(state), hbm(gate_blocks.reshape(X, M, 8, W)), hbm(gate_slot.reshape(1, Z * X)))
    packed = exchange(packed, ("z", "x"), ZX_ORDER)
    plane = pl.pallas_call(
        sum_kernel,
        out_shape=shape((X * Y, 64, W), BF),
        in_specs=[VM, VM],
        out_specs=VM,
        scratch_shapes=[pltpu.VMEM((32, W), F32)],
        compiler_params=CP, name="sum",
    )(slots, packed)
    plane = exchange(plane, ("x", "y"), XY_ORDER)
    pair = lax.ppermute(plane, "k", [(0, 1), (1, 0)])
    hot = pl.pallas_call(
        hot_kernel,
        out_shape=shape((2 * W, 4096), BF),
        in_specs=[VM, ANY],
        out_specs=VM,
        compiler_params=CP,
        cost_estimate=pl.CostEstimate(flops=2**22, bytes_accessed=2**21, transcendentals=0),
        name="hot",
    )(samples, plane)
    amplitudes, picked = pl.pallas_call(
        apply_kernel,
        out_shape=(shape((1, 16, 2, W), F32), shape((Z, 40, W), BF)),
        in_specs=[VM, VM, VM, VM],
        out_specs=(VM, VM),
        scratch_shapes=[pltpu.VMEM((X * Y, K, 64, W), BF), pltpu.VMEM((X, 2, W, W), F32), pltpu.VMEM((32, W), F32)],
        compiler_params=CP, name="apply",
    )(samples, hot, plane, pair)
    picked = exchange(picked, "z", Z_ORDER)
    probs, score, amplitudes = pl.pallas_call(
        finish_kernel,
        out_shape=(shape((Z, 4096), F32), shape((1, Z), F32), shape((1, 16, 2, W), F32)),
        in_specs=[VM, VM],
        out_specs=(VM, VM, VM),
        scratch_shapes=[pltpu.VMEM((Z * 32, W), F32)],
        compiler_params=CP, name="finish",
    )(picked, amplitudes)
    return amplitudes, probs, score.reshape(Z)


def solution(mesh):
    split = Mesh(mesh.devices.reshape(Z, X, Y, K), ("z", "x", "y", "k"))
    placed = (P(None, ("z", "x"), None, ("y", "k"), None, None), P(("z", "x"), None, None, None), P(), P())
    return jax.shard_map(
        on_device,
        mesh=split,
        in_specs=placed,
        out_specs=(P(("z", "x"), ("y", "k"), None, None), P(), P()),
        check_vma=False,
    )
```
